32 devices in a mesh: owner: 4 (over y, x), rows: 8 (over z, core).
Axes of the slice: x: 2, y: 2, z: 4, core: 2. Of those that a mesh axis runs over, the one named last changes fastest.
Arguments:
- train_gate: float32 [128, 2048, 768], P('owner', 'rows'), may hold values from -0.1875 to 0.1875
- other_gate: bfloat16 [128, 2048, 768], P('owner', 'rows'), may hold values from -0.0625 to 0.0625
- train_up: float32 [128, 2048, 768], P('owner', 'rows'), may hold values from -0.1875 to 0.1875
- other_up: bfloat16 [128, 2048, 768], P('owner', 'rows'), may hold values from -0.0625 to 0.0625
- router_weight: float32 [2048, 128], P('rows', 'owner'), may hold values from -0.125 to 0.125
- router_gain: float32 [2048], P('rows'), may hold values from 0.25 to 1.75
Outputs:
- ready_gate: bfloat16 [128, 2048, 768], P(('owner', 'rows'))
- ready_up: bfloat16 [128, 2048, 768], P(('owner', 'rows'))
- scale_gate: float32 [128, 768], P(('owner', 'rows'))
- scale_up: float32 [128, 768], P(('owner', 'rows'))
- serve_router: bfloat16 [2048, 128], replicated
The draws below stay inside these ranges and needn't reach their ends.
All inputs are finite; a program needn't handle non-finite values. Where the reference program divides by a largest or mean magnitude, that divisor is 1e-20 or more.
Results may differ from the reference program's by a relative error of at most 0.001.
Values may be sent and summed in bfloat16 or wider, within the bound.
A program may use at most 192 MiB of HBM per device.

```python
import jax
import jax.numpy as jnp

EXPERTS = 128
D_MODEL = 2048
D_EXPERT = 768


def strengthened(entries, stream_key, source, target, shards_of, factor):
    def block_of(position):
        return (jnp.arange(entries.shape[position]) // (entries.shape[position] // shards_of)).reshape((-1,) + (1,) * (entries.ndim - 1 - position))

    first = jax.random.permutation(stream_key, shards_of)[block_of(target)]
    other_side = (block_of(target) + shards_of // 2) % shards_of
    return jnp.where((block_of(source) == first) | (block_of(source) == other_side), factor * entries, entries)


def steps_of(rng, extent, split, least, largest):
    loudness, own = 1.0, jax.random.fold_in(rng, 6)
    for axis_at, blocks in split:
        heights = jnp.exp(jax.random.uniform(jax.random.fold_in(own, axis_at), (blocks,), jnp.float32, least / len(split), largest / len(split)))
        loudness = loudness * jnp.repeat(heights, extent[axis_at] // blocks).reshape([-1 if axis == axis_at else 1 for axis in range(len(extent))])
    return loudness


def noise(own_key, shape, width, reach, pieces=(), dtype=jnp.bfloat16):
    drawn = width * jax.random.normal(own_key, shape, jnp.float32)
    if pieces:
        drawn = drawn * steps_of(own_key, shape, pieces, -0.22, 0.18)
    return jnp.clip(drawn, -reach, reach).astype(dtype)


def noise_with(own_key, shape, width, most, split, heavy, dtype=jnp.bfloat16):
    entries = width * jax.random.normal(own_key, shape, jnp.float32)
    if split:
        entries = entries * steps_of(own_key, shape, split, -0.22, 0.18)
    return jnp.clip(strengthened(entries, jax.random.fold_in(own_key, 3), *heavy), -most, most).astype(dtype)


def setup_inputs(seed: int = 0) -> dict:
    key_list = jax.random.split(jax.random.key(seed), 7)
    return {
        "train_gate": noise_with(key_list[0], (EXPERTS, D_MODEL, D_EXPERT), D_MODEL ** -0.5, 0.1875, ((0, 4), (1, 8)), (1, 2, 8, 2.0), jnp.float32),
        "other_gate": noise(key_list[1], (EXPERTS, D_MODEL, D_EXPERT), (D_MODEL * 4) ** -0.5, 0.0625, ((0, 4), (1, 8))),
        "train_up": noise_with(key_list[2], (EXPERTS, D_MODEL, D_EXPERT), D_MODEL ** -0.5, 0.1875, ((0, 4), (1, 8)), (1, 2, 8, 2.0), jnp.float32),
        "other_up": noise(key_list[3], (EXPERTS, D_MODEL, D_EXPERT), (D_MODEL * 4) ** -0.5, 0.0625, ((0, 4), (1, 8))),
        "router_weight": noise(key_list[4], (D_MODEL, EXPERTS), D_MODEL ** -0.5, 0.125, ((0, 8), (1, 4)), jnp.float32),
        "router_gain": jnp.clip(1.0 + 0.15 * jax.random.normal(key_list[5], (D_MODEL,), jnp.float32), 0.25, 1.75),
    }


def reference(train_gate, other_gate, train_up, other_up, router_weight, router_gain):
    latest_gate = train_gate + other_gate.astype(jnp.float32)
    latest_up = train_up + other_up.astype(jnp.float32)
    scale_gate = jnp.max(jnp.abs(latest_gate), axis=1)
    ready_gate = (latest_gate / jnp.expand_dims(scale_gate, 1)).astype(jnp.bfloat16)
    scale_up = jnp.max(jnp.abs(latest_up), axis=1)
    ready_up = (latest_up / jnp.expand_dims(scale_up, 1)).astype(jnp.bfloat16)
    serve_router = (router_weight * router_gain[:, None]).astype(jnp.bfloat16)
    return ready_gate, ready_up, scale_gate, scale_up, serve_router
```

```python
import functools

import jax
import jax.numpy as jnp
from jax import lax
from jax.experimental import pallas as pl
from jax.experimental.pallas import tpu as pltpu
from jax.sharding import PartitionSpec as P

F32, BF16 = jnp.float32, jnp.bfloat16
CHUNK = 32
AHEAD = 4


def flipped(me, k, n):
    out, bit = 0, 1
    while bit < n:
        out = out + ((me // bit + k // bit) % 2) * bit
        bit *= 2
    return out


def kernel(n, owners, each, train_gate, other_gate, train_up, other_up, part_router,
           ready_gate, ready_up, scale_gate, scale_up, router,
           wide, narrow, send, maxes, gathered, halves, mirrored, full, padded, pieces,
           load_sem, send_sem, recv_sem,
           as_sem, ar_sem, bs_sem, br_sem, cs_sem, cr_sem,
           r1_send, r1_recv, r2_send, r2_recv, r3_send, r3_recv, r4_send, r4_recv, r5_send, r5_recv):
    me, owner = lax.axis_index("rows"), lax.axis_index("owner")
    rows = wide.shape[2]
    units = 2 * each
    half = n // 2
    spot = me % half
    base = me - spot
    mirror = (me + half) % n
    slots = send.shape[0]
    trains, others, readies = (train_gate, train_up), (other_gate, other_up), (ready_gate, ready_up)
    scales = (scale_gate, scale_up)

    def remote(src, dst, s, r, **where):
        return pltpu.make_async_remote_copy(
            src_ref=src, dst_ref=dst, send_sem=s, recv_sem=r, device_id=where,
            device_id_type=pl.DeviceIdType.MESH,
        )

    def loads(unit, d):
        kind, j, slot = unit // each, unit % each, unit % 2
        return (
            pltpu.make_async_copy(trains[kind].at[d, j], wide.at[slot, d], load_sem.at[slot, d, 0]),
            pltpu.make_async_copy(others[kind].at[d, j], narrow.at[slot, d], load_sem.at[slot, d, 1]),
        )

    def pair(k):
        return (spot + k) % half

    def start(unit):
        if unit < units:
            def one(k, _):
                for s in range(2):
                    for copy in loads(unit, 2 * pair(k) + s):
                        copy.start()
                return 0

            lax.fori_loop(1, half + 1, one, 0)

    start(0)
    barrier = pltpu.get_barrier_semaphore()
    for k in range(1, n):
        pl.semaphore_signal(barrier, inc=1, device_id={"rows": (me + k) % n},
                            device_id_type=pl.DeviceIdType.MESH)
    for k in range(1, owners):
        pl.semaphore_signal(barrier, inc=1, device_id={"owner": (owner + k) % owners},
                            device_id_type=pl.DeviceIdType.MESH)
    pl.semaphore_wait(barrier, n - 1 + owners - 1)

    def to_spot(unit, k):
        q = pair(k)
        return remote(maxes.at[unit, q], gathered.at[unit, spot], as_sem.at[unit, k],
                      ar_sem.at[unit, k], rows=base + q)

    def to_mirror(unit):
        return remote(halves.at[unit], mirrored.at[unit], bs_sem.at[unit], br_sem.at[unit], rows=mirror)

    def to_half(unit, k):
        return remote(full.at[unit, spot], full.at[unit, spot], cs_sem.at[unit, k],
                      cr_sem.at[unit, k], rows=base + pair(k))

    def maxima(unit):
        slot = unit % 2

        def largest(d):
            acc = None
            for i in range(rows // CHUNK):
                x = wide[slot, d, i * CHUNK:(i + 1) * CHUNK, :]
                y = narrow[slot, d, i * CHUNK:(i + 1) * CHUNK, :].astype(F32)
                a = jnp.abs(x + y)
                acc = a if acc is None else jnp.maximum(acc, a)
            return jnp.max(acc, axis=0, keepdims=True)

        def both(k, _):
            q = pair(k)
            for s in range(2):
                for copy in loads(unit, 2 * q + s):
                    copy.wait()
                maxes[unit, q, s:s + 1, :] = largest(2 * q + s)
            return 0

        def shared(k, _):
            both(k, 0)
            to_spot(unit, k).start()
            return 0

        lax.fori_loop(1, half, shared, 0)
        both(0, 0)
        gathered[unit, spot] = maxes[unit, spot]

    def exchange(unit):
        kind, j = unit // each, unit % each
        for k in range(1, half):
            to_spot(unit, k).wait()
        mine = gathered[unit, 0]
        for q in range(1, half):
            mine = jnp.maximum(mine, gathered[unit, q])
        halves[unit] = mine
        to_mirror(unit).start()
        to_mirror(unit).wait()
        full[unit, spot] = jnp.maximum(mine, mirrored[unit])
        for k in range(1, half):
            to_half(unit, k).start()
        for k in range(1, half):
            to_half(unit, k).wait()
        scales[kind][j:j + 1, :] = scale_of(unit, me)

    def scale_of(unit, d):
        two = full[unit, d // 2]
        return jnp.where(d % 2 == 0, two[0:1], two[1:2])

    far, near = list(range(n // 2, n)), list(range(2, n // 2))
    side = me % 2

    def dest(p):
        a, b, c = len(far), len(near), n // 2
        in_far = jnp.where(side == 0, p < a, jnp.logical_and(p >= b, p < a + b))
        at_far = p - side * b
        at_near = p - (1 - side) * a
        k = jnp.where(p == n - 2, 1, jnp.where(in_far, c + at_far, 2 + at_near))
        return flipped(me, k, n)

    def data(unit, p, d):
        kind, j, slot = unit // each, unit % each, unit % slots
        return remote(send.at[slot, p], readies[kind].at[j, me], send_sem.at[slot, p],
                      recv_sem.at[unit, me], rows=d)

    def blocks(unit):
        slot = unit % 2
        kind, j = unit // each, unit % each

        def scaled(d, put):
            inverse = 1.0 / scale_of(unit, d)
            for i in range(rows // CHUNK):
                x = wide[slot, d, i * CHUNK:(i + 1) * CHUNK, :]
                y = narrow[slot, d, i * CHUNK:(i + 1) * CHUNK, :].astype(F32)
                put(slice(i * CHUNK, (i + 1) * CHUNK), ((x + y) * inverse).astype(BF16))

        def one(p, _):
            d = dest(p)
            if unit >= slots:
                data(unit - slots, p, d).wait_send()

            def put(at, value):
                send[unit % slots, p, at, :] = value

            scaled(d, put)
            data(unit, p, d).start()
            return 0

        lax.fori_loop(0, n - 1, one, 0)

        def put(at, value):
            readies[kind][j, me, at, :] = value

        scaled(me, put)

    rows_of = rows // owners

    def block_of(r):
        return pl.ds(pl.multiple_of(r * rows, rows), rows)

    def share_of(r, o):
        return pl.ds(pl.multiple_of(r * rows + o * rows_of, rows_of), rows_of)

    def r1(k):
        return remote(padded, pieces.at[owner], r1_send.at[k], r1_recv.at[k], owner=(owner + k) % owners)

    def r2(k):
        at = router.at[block_of(me)]
        return remote(at, at, r2_send.at[k], r2_recv.at[k], rows=base + pair(k))

    def r3():
        at = router.at[share_of(me, owner)]
        return remote(at, at, r3_send, r3_recv, rows=mirror)

    def r4(k):
        at = router.at[share_of(mirror, owner)]
        return remote(at, at, r4_send.at[k], r4_recv.at[k], owner=(owner + k) % owners)

    def r5(k):
        at = router.at[block_of(mirror)]
        return remote(at, at, r5_send.at[k], r5_recv.at[k], rows=base + pair(k))

    def router_owners():
        columns, lanes = part_router.shape[1], padded.shape[1]
        lane = lax.broadcasted_iota(jnp.int32, (columns, lanes), 1)
        row = lax.broadcasted_iota(jnp.int32, (columns, lanes), 0)
        place = (lane == row + owner * columns).astype(F32).astype(BF16)
        padded[...] = jnp.dot(part_router[...], place, preferred_element_type=F32).astype(BF16)
        pieces[owner] = padded[...]
        for k in range(1, owners):
            r1(k).start()

    def router_rows():
        for k in range(1, owners):
            r1(k).wait()
        total = pieces[0].astype(F32)
        for o in range(1, owners):
            total = total + pieces[o].astype(F32)
        router[block_of(me), :] = total.astype(BF16)
        r3().start()
        for k in range(1, half):
            r2(k).start()

    def router_across():
        r3().wait()
        for k in range(1, owners):
            r4(k).start()

    def router_far():
        for k in range(1, owners):
            r4(k).wait()
        for k in range(1, half):
            r5(k).start()

    stages = [router_owners, router_rows, router_across, router_far]
    for unit in range(units):
        maxima(unit)
        start(unit + 1)
        exchange(unit)
        blocks(unit)
        if stages:
            stages.pop(0)()
    for stage in stages:
        stage()
    for k in range(1, half):
        r2(k).wait()
        r5(k).wait()

    for unit in range(units):
        kind, j = unit // each, unit % each

        def ended(k, _, unit=unit, kind=kind, j=j):
            d = (me + k) % n
            copy = remote(send.at[unit % slots, k - 1], readies[kind].at[j, d],
                          send_sem.at[unit % slots, k - 1], recv_sem.at[unit, d], rows=d)
            if unit >= units - slots:
                copy.wait_send()
            copy.wait_recv()
            return 0

        lax.fori_loop(1, n, ended, 0)


def store(count, *refs):
    sources, results, sem = refs[:count], refs[count:2 * count], refs[2 * count]
    copies = []
    for i, (source, result) in enumerate(zip(sources, results)):
        copies.append(pltpu.make_async_copy(source, result, sem.at[i]))
    for copy in copies:
        copy.start()
    for copy in copies:
        copy.wait()


def stored(arrays):
    count = len(arrays)
    return pl.pallas_call(
        functools.partial(store, count),
        out_shape=tuple(jax.ShapeDtypeStruct(x.shape, x.dtype) for x in arrays),
        in_specs=[pl.BlockSpec(memory_space=pltpu.VMEM)] * count,
        out_specs=(pl.BlockSpec(memory_space=pl.ANY),) * count,
        scratch_shapes=[pltpu.SemaphoreType.DMA((count,))],
        compiler_params=pltpu.CompilerParams(vmem_limit_bytes=1024 * 1024),
    )(*arrays)


def per_device(n, owners, train_gate, other_gate, train_up, other_up, router_weight, router_gain):
    experts, rows, width = train_gate.shape
    each = experts // n
    units = 2 * each
    half = n // 2
    slots = min(units, AHEAD)
    columns = router_weight.shape[1]
    part = (router_weight * router_gain[:, None]).astype(BF16)
    blocks = [x.reshape(n, each, rows, width) for x in (train_gate, other_gate, train_up, other_up)]
    hbm, vmem = pl.BlockSpec(memory_space=pl.ANY), pl.BlockSpec(memory_space=pltpu.VMEM)
    dma = pltpu.SemaphoreType.DMA
    scratch = n * rows * width * (2 * 6 + slots * 2) + 4 * units * (3 * half + 2) * 2 * width * 4
    results = pl.pallas_call(
        functools.partial(kernel, n, owners, each),
        out_shape=(
            pltpu.VMEM((each, n, rows, width), BF16),
            pltpu.VMEM((each, n, rows, width), BF16),
            pltpu.VMEM((each, width), F32),
            pltpu.VMEM((each, width), F32),
            pltpu.VMEM((n * rows, owners * columns), BF16),
        ),
        in_specs=[hbm] * 4 + [vmem],
        out_specs=(vmem,) * 5,
        scratch_shapes=[
            pltpu.VMEM((2, n, rows, width), F32),
            pltpu.VMEM((2, n, rows, width), BF16),
            pltpu.VMEM((slots, n - 1, rows, width), BF16),
            pltpu.VMEM((units, half, 2, width), F32),
            pltpu.VMEM((units, half, 2, width), F32),
            pltpu.VMEM((units, 2, width), F32),
            pltpu.VMEM((units, 2, width), F32),
            pltpu.VMEM((units, half, 2, width), F32),
            pltpu.VMEM((rows, owners * columns), BF16),
            pltpu.VMEM((owners, rows, owners * columns), BF16),
            dma((2, n, 2)), dma((slots, n)), dma((units, n)),
            dma((units, half)), dma((units, half)), dma((units,)), dma((units,)),
            dma((units, half)), dma((units, half)),
            dma((owners,)), dma((owners,)), dma((half,)), dma((half,)), dma(()), dma(()),
            dma((owners,)), dma((owners,)), dma((half,)), dma((half,)),
        ],
        compiler_params=pltpu.CompilerParams(
            collective_id=0, has_side_effects=True, vmem_limit_bytes=scratch + 2 * 1024 * 1024
        ),
    )(*blocks, part)
    ready_gate, ready_up, scale_gate, scale_up, router = stored(results)
    ready_gate, ready_up = (x.reshape(each, n * rows, width) for x in (ready_gate, ready_up))
    return (ready_gate, ready_up, scale_gate, scale_up, router)


def solution(mesh):
    n, owners = mesh.shape["rows"], mesh.shape["owner"]
    in_specs = (
        P("owner", "rows", None),
        P("owner", "rows", None),
        P("owner", "rows", None),
        P("owner", "rows", None),
        P("rows", "owner"),
        P("rows"),
    )
    out_specs = (
        P(("owner", "rows"), None, None),
        P(("owner", "rows"), None, None),
        P(("owner", "rows"), None),
        P(("owner", "rows"), None),
        P(),
    )
    return jax.shard_map(
        functools.partial(per_device, n, owners), mesh=mesh, in_specs=in_specs,
        out_specs=out_specs, check_vma=False,
    )
```

```python
import functools

import jax
import jax.numpy as jnp
from jax import lax
from jax.experimental import pallas as pl
from jax.experimental.pallas import tpu as pltpu
from jax.sharding import PartitionSpec as P

F32, BF16 = jnp.float32, jnp.bfloat16
CHUNK = 32
PARTS, FAR_DEEP, NEAR_DEEP, SPLIT = 4, 3, 4, 2


def flipped(me, k, n):
    out, bit = 0, 1
    while bit < n:
        out = out + ((me // bit + k // bit) % 2) * bit
        bit *= 2
    return out


def kernel(n, owners, each, train_gate, other_gate, train_up, other_up, router_weight, router_gain,
           ready_gate, ready_up, scale_gate, scale_up, router,
           wide, narrow, send, maxes, gathered, halves, mirrored, full, solo, direct,
           weight, gain, padded, pieces,
           load_sem, send_sem, recv_sem, ds_sem, dr_sem, router_sem,
           as_sem, ar_sem, bs_sem, br_sem, cs_sem, cr_sem,
           r1_send, r1_recv, r2_send, r2_recv, r3_send, r3_recv, r4_send, r4_recv, r5_send, r5_recv):
    me, owner = lax.axis_index("rows"), lax.axis_index("owner")
    rows = wide.shape[2]
    units = 2 * each
    half = n // 2
    spot = me % half
    base = me - spot
    mirror = (me + half) % n
    deep = send.shape[0]
    part = send.shape[1]
    parts = rows // part
    trains, others, readies = (train_gate, train_up), (other_gate, other_up), (ready_gate, ready_up)
    scales = (scale_gate, scale_up)

    def remote(src, dst, s, r, **where):
        return pltpu.make_async_remote_copy(
            src_ref=src, dst_ref=dst, send_sem=s, recv_sem=r, device_id=where,
            device_id_type=pl.DeviceIdType.MESH,
        )

    def loads(unit, q):
        kind, j, slot = unit // each, unit % each, unit % 2
        two = pl.ds(2 * q, 2)
        return (
            pltpu.make_async_copy(trains[kind].at[two, j], wide.at[slot, two], load_sem.at[slot, q, 0]),
            pltpu.make_async_copy(others[kind].at[two, j], narrow.at[slot, two], load_sem.at[slot, q, 1]),
        )

    def pair(k):
        return (spot + k) % half

    def start(unit):
        if unit < units:
            def one(k, _):
                for copy in loads(unit, pair(k)):
                    copy.start()
                return 0

            lax.fori_loop(1, half + 1, one, 0)

    start(0)
    barrier = pltpu.get_barrier_semaphore()
    for k in range(1, n):
        pl.semaphore_signal(barrier, inc=1, device_id={"rows": (me + k) % n},
                            device_id_type=pl.DeviceIdType.MESH)
    for k in range(1, owners):
        pl.semaphore_signal(barrier, inc=1, device_id={"owner": (owner + k) % owners},
                            device_id_type=pl.DeviceIdType.MESH)
    routing = (pltpu.make_async_copy(router_weight, weight, router_sem.at[0]),
               pltpu.make_async_copy(router_gain, gain, router_sem.at[1]))
    for copy in routing:
        copy.start()

    def to_spot(unit, k):
        q = pair(k)
        return remote(maxes.at[unit, q], gathered.at[unit, spot], as_sem.at[k],
                      ar_sem.at[k], rows=base + q)

    def to_mirror(unit):
        return remote(halves.at[unit], mirrored.at[unit], bs_sem.at[unit % 2], br_sem.at[unit % 2], rows=mirror)

    def to_half(unit, k):
        return remote(full.at[unit, spot], full.at[unit, spot], cs_sem.at[k],
                      cr_sem.at[k], rows=base + pair(k))

    def maxima(unit):
        slot = unit % 2

        def largest(d):
            acc = None
            for i in range(rows // CHUNK):
                x = wide[slot, d, i * CHUNK:(i + 1) * CHUNK, :]
                y = narrow[slot, d, i * CHUNK:(i + 1) * CHUNK, :].astype(F32)
                a = jnp.abs(x + y)
                acc = a if acc is None else jnp.maximum(acc, a)
            return jnp.max(acc, axis=0, keepdims=True)

        def both(k, _):
            q = pair(k)
            for copy in loads(unit, q):
                copy.wait()
            for s in range(2):
                d = 2 * q + s
                most = largest(d)
                maxes[unit, q, s:s + 1, :] = most
                if unit == 0:
                    solo[d] = most
            return 0

        def shared(k, _):
            both(k, 0)
            if unit > 0:
                to_spot(unit, k).start()
            return 0

        lax.fori_loop(1, half, shared, 0)
        both(0, 0)
        gathered[unit, spot] = maxes[unit, spot]
        if unit == 0:
            direct[me] = solo[mirror]

    def to_direct(k):
        r = (me + k) % n
        return remote(solo.at[(r + half) % n], direct.at[me], ds_sem.at[k], dr_sem.at[k], rows=r)

    def first_scale():
        for k in range(1, n):
            to_direct(k).wait()
        total = direct[0]
        for d in range(1, n):
            total = jnp.maximum(total, direct[d])
        return total

    def across(unit):
        for k in range(1, half):
            to_spot(unit, k).wait()
        mine = gathered[unit, 0]
        for q in range(1, half):
            mine = jnp.maximum(mine, gathered[unit, q])
        halves[unit] = mine
        to_mirror(unit).start()

    def spread(unit):
        to_mirror(unit).wait()
        full[unit, spot] = jnp.maximum(halves[unit], mirrored[unit])
        for k in range(1, half):
            to_half(unit, k).start()

    def known(unit):
        kind, j = unit // each, unit % each
        for k in range(1, half):
            to_half(unit, k).wait()
        scales[kind][j:j + 1, :] = scale_of(unit, me)

    def scale_of(unit, d):
        two = full[unit, d // 2]
        return jnp.where(d % 2 == 0, two[0:1], two[1:2])

    far_items, near_items = half * parts, (half - 2) * parts
    items = far_items + near_items + parts
    side = me % 2

    def item(unit, t):
        lead = parts if unit == 0 else 0
        mixed = far_items - lead + near_items
        after = jnp.maximum(t - lead, 0)
        phase = side * (2 * mixed // 3)
        near_at = (after * near_items + phase) // mixed
        leading, beside = t < lead, t >= lead + mixed
        is_far = jnp.logical_or(leading, jnp.logical_and(
            jnp.logical_not(beside), ((after + 1) * near_items + phase) // mixed == near_at))
        far_at = jnp.where(leading, t, lead + after - near_at)
        near_at = jnp.where(beside, near_items + t - lead - mixed, near_at)
        at = jnp.where(is_far, far_at, near_at)
        near_k = jnp.where(beside, 1, 2 + at // parts)
        d = flipped(me, jnp.where(is_far, half + at // parts, near_k), n)
        slot = jnp.where(is_far, (unit * far_items + far_at) % FAR_DEEP,
                         FAR_DEEP + (unit * (near_items + parts) + near_at) % NEAR_DEEP)
        fresh = at < jnp.where(is_far, FAR_DEEP, NEAR_DEEP)
        return d, at % parts, slot, fresh

    def part_of(piece):
        return pl.ds(pl.multiple_of(piece * part, part), part)

    def data(unit, d, piece, slot):
        kind, j = unit // each, unit % each
        return remote(send.at[slot], readies[kind].at[j, me, part_of(piece)], send_sem.at[slot],
                      recv_sem.at[kind, me], rows=d)

    def scaled(unit, d, piece, put, scale=None):
        inverse = 1.0 / (scale_of(unit, d) if scale is None else scale)
        chunk = min(CHUNK, part)
        for i in range(part // chunk):
            at = pl.ds(pl.multiple_of(piece * part + i * chunk, chunk), chunk)
            x = wide[unit % 2, d, at, :]
            y = narrow[unit % 2, d, at, :].astype(F32)
            put(i * chunk, chunk, ((x + y) * inverse).astype(BF16))

    def issue(unit, first, last, scale=None):
        def one(t, _):
            d, piece, slot, fresh = item(unit, t)
            if unit == 0:
                @pl.when(jnp.logical_not(fresh))
                def _():
                    data(unit, d, piece, slot).wait_send()
            else:
                data(unit, d, piece, slot).wait_send()

            def put(at, size, value):
                send[slot, at:at + size, :] = value

            scaled(unit, d, piece, put, scale)
            data(unit, d, piece, slot).start()
            return 0

        lax.fori_loop(first, last, one, 0)

    def own(unit):
        kind, j = unit // each, unit % each

        def one(piece, _):
            def put(at, size, value):
                readies[kind][j, me, pl.ds(pl.multiple_of(piece * part + at, size), size), :] = value

            scaled(unit, me, piece, put)
            return 0

        lax.fori_loop(0, parts, one, 0)

    rows_of = rows // owners

    def block_of(r):
        return pl.ds(pl.multiple_of(r * rows, rows), rows)

    def share_of(r, o):
        return pl.ds(pl.multiple_of(r * rows + o * rows_of, rows_of), rows_of)

    def r1(k):
        return remote(padded, pieces.at[owner], r1_send.at[k], r1_recv.at[k], owner=(owner + k) % owners)

    def r2(k):
        at = router.at[block_of(me)]
        return remote(at, at, r2_send.at[k], r2_recv.at[k], rows=base + pair(k))

    def r3():
        at = router.at[share_of(me, owner)]
        return remote(at, at, r3_send, r3_recv, rows=mirror)

    def r4(k):
        at = router.at[share_of(mirror, owner)]
        return remote(at, at, r4_send.at[k], r4_recv.at[k], owner=(owner + k) % owners)

    def r5(k):
        at = router.at[block_of(mirror)]
        return remote(at, at, r5_send.at[k], r5_recv.at[k], rows=base + pair(k))

    def router_owners():
        for copy in routing:
            copy.wait()
        columns, lanes = weight.shape[0], padded.shape[1]
        lane = lax.broadcasted_iota(jnp.int32, (columns, lanes), 1)
        row = lax.broadcasted_iota(jnp.int32, (columns, lanes), 0)
        place = (lane == row + owner * columns).astype(F32).astype(BF16)
        mine = (weight[...] * gain[...]).astype(BF16)
        padded[...] = lax.dot_general(mine, place, (((0,), (0,)), ((), ())),
                                      preferred_element_type=F32).astype(BF16)
        pieces[owner] = padded[...]
        for k in range(1, owners):
            r1(k).start()

    def router_rows():
        for k in range(1, owners):
            r1(k).wait()
        total = pieces[0].astype(F32)
        for o in range(1, owners):
            total = total + pieces[o].astype(F32)
        router[block_of(me), :] = total.astype(BF16)
        r3().start()
        for k in range(1, half):
            r2(k).start()

    def router_across():
        r3().wait()
        for k in range(1, owners):
            r4(k).start()

    def router_far():
        for k in range(1, owners):
            r4(k).wait()
        for k in range(1, half):
            r5(k).start()

    maxima(0)
    pl.semaphore_wait(barrier, n - 1 + owners - 1)
    for k in range(1, half):
        to_spot(0, k).start()
    for k in range(1, n):
        to_direct(k).start()
    start(1)
    across(0)
    now = min(FAR_DEEP, parts)
    first = first_scale()
    issue(0, 0, now, first)
    spread(0)
    issue(0, now, parts, first)
    known(0)
    stages = [router_owners, router_rows, router_across, router_far]
    steps = (maxima, across, spread)
    for unit in range(units):
        more = unit + 1 < units
        at = parts if unit == 0 else 0
        marks = [at + (items - at) * mark // 28 for mark in (2, 9, 16)]
        for mark, step in zip(marks, steps):
            issue(unit, at, mark)
            at = mark
            if more:
                step(unit + 1)
        issue(unit, at, items)
        own(unit)
        start(unit + 2)
        if more:
            known(unit + 1)
        if stages:
            stages.pop(0)()
    for stage in stages:
        stage()
    for k in range(1, half):
        r2(k).wait()
        r5(k).wait()
    for slot in range(deep):
        data(0, mirror, 0, slot).wait_send()
    for kind in range(2):
        def ended(k, _, kind=kind):
            d = (me + k) % n
            at = readies[kind].at[:, d]
            remote(at, at, send_sem.at[0], recv_sem.at[kind, d], rows=d).wait_recv()
            return 0

        lax.fori_loop(1, n, ended, 0)


def store(count, *refs):
    sources, results, sem = refs[:count], refs[count:2 * count], refs[2 * count]
    copies = []
    for source, result in zip(sources, results):
        whole = len(source.shape) < 4
        for at in range(1 if whole else source.shape[0] * SPLIT):
            if not whole:
                size = source.shape[1] // SPLIT
                index = (at // SPLIT, pl.ds(at % SPLIT * size, size))
            pieces = (source, result) if whole else (source.at[index], result.at[index])
            copies.append(pltpu.make_async_copy(*pieces, sem.at[len(copies)]))
    for copy in copies:
        copy.start()
    for copy in copies:
        copy.wait()


def stored(arrays):
    count = len(arrays)
    copies = sum(x.shape[0] * SPLIT if x.ndim == 4 else 1 for x in arrays)
    return pl.pallas_call(
        functools.partial(store, count),
        out_shape=tuple(jax.ShapeDtypeStruct(x.shape, x.dtype) for x in arrays),
        in_specs=[pl.BlockSpec(memory_space=pltpu.VMEM)] * count,
        out_specs=(pl.BlockSpec(memory_space=pl.ANY),) * count,
        scratch_shapes=[pltpu.SemaphoreType.DMA((copies,))],
        compiler_params=pltpu.CompilerParams(vmem_limit_bytes=1024 * 1024),
    )(*arrays)


def per_device(n, owners, train_gate, other_gate, train_up, other_up, router_weight, router_gain):
    experts, rows, width = train_gate.shape
    each = experts // n
    units = 2 * each
    half = n // 2
    part = rows // PARTS
    deep = FAR_DEEP + NEAR_DEEP
    columns = router_weight.shape[1]
    blocks = [x.reshape(n, each, rows, width) for x in (train_gate, other_gate, train_up, other_up)]
    hbm, vmem = pl.BlockSpec(memory_space=pl.ANY), pl.BlockSpec(memory_space=pltpu.VMEM)
    dma = pltpu.SemaphoreType.DMA
    scratch = n * rows * width * 12 + deep * part * width * 2 + units * (3 * half + 2) * 2 * width * 4
    results = pl.pallas_call(
        functools.partial(kernel, n, owners, each),
        out_shape=(
            pltpu.VMEM((each, n, rows, width), BF16),
            pltpu.VMEM((each, n, rows, width), BF16),
            pltpu.VMEM((each, width), F32),
            pltpu.VMEM((each, width), F32),
            pltpu.VMEM((n * rows, owners * columns), BF16),
        ),
        in_specs=[hbm] * 4 + [pl.BlockSpec(memory_space=pltpu.HBM)] * 2,
        out_specs=(vmem,) * 5,
        scratch_shapes=[
            pltpu.VMEM((2, n, rows, width), F32),
            pltpu.VMEM((2, n, rows, width), BF16),
            pltpu.VMEM((deep, part, width), BF16),
            pltpu.VMEM((units, half, 2, width), F32),
            pltpu.VMEM((units, half, 2, width), F32),
            pltpu.VMEM((units, 2, width), F32),
            pltpu.VMEM((units, 2, width), F32),
            pltpu.VMEM((units, half, 2, width), F32),
            pltpu.VMEM((n, 1, width), F32),
            pltpu.VMEM((n, 1, width), F32),
            pltpu.VMEM((columns, rows), F32),
            pltpu.VMEM((1, rows), F32),
            pltpu.VMEM((rows, owners * columns), BF16),
            pltpu.VMEM((owners, rows, owners * columns), BF16),
            dma((2, half, 2)), dma((deep,)), dma((2, n)),
            dma((n,)), dma((n,)), dma((2,)),
            dma((half,)), dma((half,)), dma((2,)), dma((2,)), dma((half,)), dma((half,)),
            dma((owners,)), dma((owners,)), dma((half,)), dma((half,)), dma(()), dma(()),
            dma((owners,)), dma((owners,)), dma((half,)), dma((half,)),
        ],
        compiler_params=pltpu.CompilerParams(
            collective_id=0, has_side_effects=True, vmem_limit_bytes=scratch + 4 * 1024 * 1024
        ),
    )(*blocks, router_weight.T, router_gain.reshape(1, rows))
    ready_gate, ready_up, scale_gate, scale_up, router = stored(results)
    ready_gate, ready_up = (x.reshape(each, n * rows, width) for x in (ready_gate, ready_up))
    return (ready_gate, ready_up, scale_gate, scale_up, router)


def solution(mesh):
    n, owners = mesh.shape["rows"], mesh.shape["owner"]
    in_specs = (
        P("owner", "rows", None),
        P("owner", "rows", None),
        P("owner", "rows", None),
        P("owner", "rows", None),
        P("rows", "owner"),
        P("rows"),
    )
    out_specs = (
        P(("owner", "rows"), None, None),
        P(("owner", "rows"), None, None),
        P(("owner", "rows"), None),
        P(("owner", "rows"), None),
        P(),
    )
    return jax.shard_map(
        functools.partial(per_device, n, owners), mesh=mesh, in_specs=in_specs,
        out_specs=out_specs, check_vma=False,
    )
```

```python
import functools

import jax
import jax.numpy as jnp
from jax import lax
from jax.experimental import pallas as pl
from jax.experimental.pallas import tpu as pltpu
from jax.sharding import PartitionSpec as P

F32, BF16 = jnp.float32, jnp.bfloat16
CHUNK = 32
PARTS, FAR_DEEP, NEAR_DEEP, SPLIT, COMMON = 4, 3, 4, 2, 6


def flipped(me, k, n):
    out, bit = 0, 1
    while bit < n:
        out = out + ((me // bit + k // bit) % 2) * bit
        bit *= 2
    return out


def kernel(n, owners, each, train_gate, other_gate, train_up, other_up, router_weight, router_gain,
           ready_gate, ready_up, scale_gate, scale_up, router, rest,
           wide, narrow, send, maxes, gathered, halves, mirrored, full, solo, direct,
           weight, gain, padded, pieces,
           load_sem, send_sem, recv_sem, gate_sem, ds_sem, dr_sem, router_sem,
           as_sem, ar_sem, bs_sem, br_sem, cs_sem, cr_sem,
           r1_send, r1_recv, r2_send, r2_recv, r3_send, r3_recv, r4_send, r4_recv, r5_send, r5_recv):
    me, owner = lax.axis_index("rows"), lax.axis_index("owner")
    rows = wide.shape[2]
    units = 2 * each
    half = n // 2
    spot = me % half
    base = me - spot
    mirror = (me + half) % n
    deep = send.shape[0]
    part = send.shape[1]
    parts = rows // part
    trains, others, readies = (train_gate, train_up), (other_gate, other_up), (ready_gate, ready_up)
    scales = (scale_gate, scale_up)

    def remote(src, dst, s, r, **where):
        return pltpu.make_async_remote_copy(
            src_ref=src, dst_ref=dst, send_sem=s, recv_sem=r, device_id=where,
            device_id_type=pl.DeviceIdType.MESH,
        )

    def loads(unit, q):
        kind, j, slot = unit // each, unit % each, unit % 2
        two = pl.ds(2 * q, 2)
        return (
            pltpu.make_async_copy(trains[kind].at[two, j], wide.at[slot, two], load_sem.at[slot, q, 0]),
            pltpu.make_async_copy(others[kind].at[two, j], narrow.at[slot, two], load_sem.at[slot, q, 1]),
        )

    def pair(k):
        return (spot + k) % half

    def start(unit):
        if unit < units:
            def one(k, _):
                for copy in loads(unit, pair(k)):
                    copy.start()
                return 0

            lax.fori_loop(1, half + 1, one, 0)

    start(0)
    barrier = pltpu.get_barrier_semaphore()
    for k in range(1, n):
        pl.semaphore_signal(barrier, inc=1, device_id={"rows": (me + k) % n},
                            device_id_type=pl.DeviceIdType.MESH)
    for k in range(1, owners):
        pl.semaphore_signal(barrier, inc=1, device_id={"owner": (owner + k) % owners},
                            device_id_type=pl.DeviceIdType.MESH)
    routing = (pltpu.make_async_copy(router_weight, weight, router_sem.at[0]),
               pltpu.make_async_copy(router_gain, gain, router_sem.at[1]))
    for copy in routing:
        copy.start()

    def to_spot(unit, k):
        q = pair(k)
        return remote(maxes.at[unit, q], gathered.at[unit, spot], as_sem.at[k],
                      ar_sem.at[k], rows=base + q)

    def to_mirror(unit):
        return remote(halves.at[unit], mirrored.at[unit], bs_sem.at[unit % 2], br_sem.at[unit % 2], rows=mirror)

    def to_half(unit, k):
        return remote(full.at[unit, spot], full.at[unit, spot], cs_sem.at[k],
                      cr_sem.at[k], rows=base + pair(k))

    def maxima(unit):
        slot = unit % 2

        def largest(d):
            acc = None
            for i in range(rows // CHUNK):
                x = wide[slot, d, i * CHUNK:(i + 1) * CHUNK, :]
                y = narrow[slot, d, i * CHUNK:(i + 1) * CHUNK, :].astype(F32)
                a = jnp.abs(x + y)
                acc = a if acc is None else jnp.maximum(acc, a)
            return jnp.max(acc, axis=0, keepdims=True)

        def both(k, _):
            q = pair(k)
            for copy in loads(unit, q):
                copy.wait()
            for s in range(2):
                d = 2 * q + s
                most = largest(d)
                maxes[unit, q, s:s + 1, :] = most
                if unit == 0:
                    solo[d] = most
            return 0

        def shared(k, _):
            both(k, 0)
            if unit > 0:
                to_spot(unit, k).start()
            return 0

        lax.fori_loop(1, half, shared, 0)
        both(0, 0)
        gathered[unit, spot] = maxes[unit, spot]
        if unit == 0:
            direct[me] = solo[mirror]

    def to_direct(k):
        r = (me + k) % n
        return remote(solo.at[(r + half) % n], direct.at[me], ds_sem.at[k], dr_sem.at[k], rows=r)

    def first_scale():
        for k in range(1, n):
            to_direct(k).wait()
        total = direct[0]
        for d in range(1, n):
            total = jnp.maximum(total, direct[d])
        return total

    def across(unit):
        for k in range(1, half):
            to_spot(unit, k).wait()
        mine = gathered[unit, 0]
        for q in range(1, half):
            mine = jnp.maximum(mine, gathered[unit, q])
        halves[unit] = mine
        to_mirror(unit).start()

    def spread(unit):
        to_mirror(unit).wait()
        full[unit, spot] = jnp.maximum(halves[unit], mirrored[unit])
        for k in range(1, half):
            to_half(unit, k).start()

    def known(unit):
        kind, j = unit // each, unit % each
        for k in range(1, half):
            to_half(unit, k).wait()
        scales[kind][j:j + 1, :] = scale_of(unit, me)

    def scale_of(unit, d):
        two = full[unit, d // 2]
        return jnp.where(d % 2 == 0, two[0:1], two[1:2])

    far_items, near_items = half * parts, (half - 2) * parts
    late = far_items // 2
    side = me % 2
    quarter = me // (half // 2)
    inner = jnp.logical_or(quarter == 1, quarter == 2)

    def far_count(unit):
        return far_items if unit < units - 2 else far_items - late

    def far_base(unit):
        return sum(far_count(u) for u in range(unit))

    def item_count(unit):
        return far_count(unit) + near_items + parts

    def item(unit, t):
        lead = parts if unit == 0 else 0
        mixed = far_count(unit) - lead + near_items
        after = jnp.maximum(t - lead, 0)
        phase = side * (2 * mixed // 3)
        near_at = (after * near_items + phase) // mixed
        leading, beside = t < lead, t >= lead + mixed
        is_far = jnp.logical_or(leading, jnp.logical_and(
            jnp.logical_not(beside), ((after + 1) * near_items + phase) // mixed == near_at))
        far_at = jnp.where(leading, t, lead + after - near_at)
        near_at = jnp.where(beside, near_items + t - lead - mixed, near_at)
        at = jnp.where(is_far, far_at, near_at)
        near_k = jnp.where(beside, 1, 2 + at // parts)
        d = flipped(me, jnp.where(is_far, half + at // parts, near_k), n)
        slot = jnp.where(is_far, (far_base(unit) + far_at) % FAR_DEEP,
                         FAR_DEEP + (unit * (near_items + parts) + near_at) % NEAR_DEEP)
        fresh = at < jnp.where(is_far, FAR_DEEP, NEAR_DEEP)
        return d, at % parts, slot, fresh

    def part_of(piece):
        return pl.ds(pl.multiple_of(piece * part, part), part)

    def data(unit, d, piece, slot):
        kind, j = unit // each, unit % each
        return remote(send.at[slot], readies[kind].at[j, me, part_of(piece)], send_sem.at[slot],
                      recv_sem.at[kind, me], rows=d)

    def scaled(unit, d, piece, put, scale=None):
        inverse = 1.0 / (scale_of(unit, d) if scale is None else scale)
        chunk = min(CHUNK, part)
        for i in range(part // chunk):
            at = pl.ds(pl.multiple_of(piece * part + i * chunk, chunk), chunk)
            x = wide[unit % 2, d, at, :]
            y = narrow[unit % 2, d, at, :].astype(F32)
            put(i * chunk, chunk, ((x + y) * inverse).astype(BF16))

    def issue(unit, first, last, scale=None):
        def one(t, _):
            d, piece, slot, fresh = item(unit, t)
            if unit == 0:
                @pl.when(jnp.logical_not(fresh))
                def _():
                    data(unit, d, piece, slot).wait_send()
            else:
                data(unit, d, piece, slot).wait_send()

            def put(at, size, value):
                send[slot, at:at + size, :] = value

            scaled(unit, d, piece, put, scale)
            data(unit, d, piece, slot).start()
            return 0

        lax.fori_loop(first, last, one, 0)

    def late_item(unit, t):
        far_at = far_items - late + t
        d = flipped(me, half + far_at // parts, n)
        return d, far_at % parts, (far_base(units) + t) % FAR_DEEP

    def issue_late(unit, first, last):
        def one(t, _):
            d, piece, slot = late_item(unit, t)
            slot = slot if unit == units - 2 else (slot + late) % FAR_DEEP
            data(unit, d, piece, slot).wait_send()

            def put(at, size, value):
                send[slot, at:at + size, :] = value

            scaled(unit, d, piece, put)
            data(unit, d, piece, slot).start()
            return 0

        lax.fori_loop(first, last, one, 0)

    def leave(unit):
        def one(t, _):
            d, piece, _ = late_item(unit, t)

            def put(at, size, value):
                rest[d % (half // 2), pl.ds(pl.multiple_of(piece * part + at, size), size), :] = value

            scaled(unit, d, piece, put)
            return 0

        lax.fori_loop(0, late, one, 0)

    def own(unit):
        kind, j = unit // each, unit % each

        def one(piece, _):
            def put(at, size, value):
                readies[kind][j, me, pl.ds(pl.multiple_of(piece * part + at, size), size), :] = value

            scaled(unit, me, piece, put)
            return 0

        lax.fori_loop(0, parts, one, 0)

    rows_of = rows // owners

    def block_of(r):
        return pl.ds(pl.multiple_of(r * rows, rows), rows)

    def share_of(r, o):
        return pl.ds(pl.multiple_of(r * rows + o * rows_of, rows_of), rows_of)

    def r1(k):
        return remote(padded, pieces.at[owner], r1_send.at[k], r1_recv.at[k], owner=(owner + k) % owners)

    def r2(k):
        at = router.at[block_of(me)]
        return remote(at, at, r2_send.at[k], r2_recv.at[k], rows=base + pair(k))

    def r3():
        at = router.at[share_of(me, owner)]
        return remote(at, at, r3_send, r3_recv, rows=mirror)

    def r4(k):
        at = router.at[share_of(mirror, owner)]
        return remote(at, at, r4_send.at[k], r4_recv.at[k], owner=(owner + k) % owners)

    def r5(k):
        at = router.at[block_of(mirror)]
        return remote(at, at, r5_send.at[k], r5_recv.at[k], rows=base + pair(k))

    def router_owners():
        for copy in routing:
            copy.wait()
        columns, lanes = weight.shape[0], padded.shape[1]
        lane = lax.broadcasted_iota(jnp.int32, (columns, lanes), 1)
        row = lax.broadcasted_iota(jnp.int32, (columns, lanes), 0)
        place = (lane == row + owner * columns).astype(F32).astype(BF16)
        mine = (weight[...] * gain[...]).astype(BF16)
        padded[...] = lax.dot_general(mine, place, (((0,), (0,)), ((), ())),
                                      preferred_element_type=F32).astype(BF16)
        pieces[owner] = padded[...]
        for k in range(1, owners):
            r1(k).start()

    def router_rows():
        for k in range(1, owners):
            r1(k).wait()
        total = pieces[0].astype(F32)
        for o in range(1, owners):
            total = total + pieces[o].astype(F32)
        router[block_of(me), :] = total.astype(BF16)
        r3().start()
        for k in range(1, half):
            r2(k).start()

    def router_across():
        r3().wait()
        for k in range(1, owners):
            r4(k).start()

    def router_far():
        for k in range(1, owners):
            r4(k).wait()
        for k in range(1, half):
            r5(k).start()

    maxima(0)
    pl.semaphore_wait(barrier, n - 1 + owners - 1)
    for k in range(1, half):
        to_spot(0, k).start()
    for k in range(1, n):
        to_direct(k).start()
    start(1)
    across(0)
    now = min(FAR_DEEP, parts)
    first = first_scale()
    issue(0, 0, now, first)
    spread(0)
    issue(0, now, parts, first)
    known(0)
    stages = [router_owners, router_rows, router_across, router_far]
    steps = (maxima, across, spread)
    for unit in range(units):
        more = unit + 1 < units
        at = parts if unit == 0 else 0
        items = item_count(unit)
        marks = [at + (items - at) * mark // 28 for mark in (2, 9, 16)]
        for mark, step in zip(marks, steps):
            issue(unit, at, mark)
            at = mark
            if more:
                step(unit + 1)
        issue(unit, at, items)
        own(unit)
        start(unit + 2)
        if more:
            known(unit + 1)
        if stages:
            stages.pop(0)()
    for stage in stages:
        stage()
    def sent(slot):
        data(0, mirror, 0, slot).wait_send()

    common = late * COMMON // 8
    issue_late(units - 2, 0, common)

    @pl.when(inner)
    def _():
        issue_late(units - 2, common, late)
        for t in range(late - FAR_DEEP, late - 1):
            sent((far_base(units) + t) % FAR_DEEP)
        pl.semaphore_signal(gate_sem, inc=1, device_id={"rows": flipped(me, half // 2, n)},
                            device_id_type=pl.DeviceIdType.MESH)
        leave(units - 1)
        sent((far_base(units) + late - 1) % FAR_DEEP)

    @pl.when(jnp.logical_not(inner))
    def _():
        pl.semaphore_wait(gate_sem, 1)
        issue_late(units - 2, common, late)
        issue_late(units - 1, 0, late)
        for slot in range(FAR_DEEP):
            sent(slot)

    for k in range(1, half):
        r2(k).wait()
        r5(k).wait()
    for slot in range(FAR_DEEP, deep):
        sent(slot)

    def landed(kind, d, count):
        at = readies[kind].at[pl.ds(0, count), d]
        remote(at, at, send_sem.at[0], recv_sem.at[kind, d], rows=d).wait_recv()

    def all_of(kind):
        def one(k, _):
            landed(kind, flipped(me, k, n), each)
            return 0
        return one

    lax.fori_loop(1, n, all_of(0), 0)
    lax.fori_loop(1, n - half // 2, all_of(1), 0)

    @pl.when(jnp.logical_not(inner))
    def _():
        lax.fori_loop(n - half // 2, n, all_of(1), 0)

    if each > 1:
        @pl.when(inner)
        def _():
            def one(k, _):
                landed(1, flipped(me, k, n), each - 1)
                return 0

            lax.fori_loop(n - half // 2, n, one, 0)


def place(n):
    me = lax.axis_index("rows")
    group = n // 4
    quarter = me // group
    return me, group, quarter, jnp.logical_or(quarter == 1, quarter == 2)


def store(n, *refs):
    count = (len(refs) - 2) // 2
    sources, results, token, sem = refs[:count], refs[count:2 * count], refs[2 * count], refs[2 * count + 1]
    token[...] = jnp.zeros_like(token)
    _, group, quarter, inner = place(n)
    copies = []

    def copy(i, index=None):
        pieces = (sources[i], results[i]) if index is None else (sources[i].at[index], results[i].at[index])
        made = pltpu.make_async_copy(*pieces, sem.at[len(copies)])
        copies.append(made)
        return made

    each = sources[0].shape[0]
    size = n // SPLIT
    whole = [copy(i) for i in range(2, count)]
    for i in range(2):
        for j in range(each if i == 0 else each - 1):
            whole += [copy(i, (j, pl.ds(at * size, size))) for at in range(SPLIT)]
    last = [copy(1, (each - 1, pl.ds(c * group, group))) for c in range(4)]
    for made in whole:
        made.start()

    def guarded(act):
        for c, made in enumerate(last):
            @pl.when(jnp.logical_not(jnp.logical_and(inner, quarter == 3 - c)))
            def _(made=made):
                act(made)

    guarded(lambda made: made.start())
    for made in whole:
        made.wait()
    guarded(lambda made: made.wait())


def stored(n, arrays):
    count = len(arrays)
    copies = count - 2 + (2 * arrays[0].shape[0] - 1) * SPLIT + 4
    return pl.pallas_call(
        functools.partial(store, n),
        out_shape=tuple(jax.ShapeDtypeStruct(x.shape, x.dtype) for x in arrays) + (pltpu.VMEM((8, 128), F32),),
        in_specs=[pl.BlockSpec(memory_space=pltpu.VMEM)] * count,
        out_specs=(pl.BlockSpec(memory_space=pl.ANY),) * count + (pl.BlockSpec(memory_space=pltpu.VMEM),),
        scratch_shapes=[pltpu.SemaphoreType.DMA((copies,))],
        compiler_params=pltpu.CompilerParams(vmem_limit_bytes=1024 * 1024),
    )(*arrays)


def swap(n, rest, _, landing, send_sem, recv_sem):
    me, group, quarter, inner = place(n)
    base = (3 - quarter) * group

    @pl.when(inner)
    def _():
        barrier = pltpu.get_barrier_semaphore()
        for i in range(group):
            pl.semaphore_signal(barrier, inc=1, device_id={"rows": base + i},
                                device_id_type=pl.DeviceIdType.MESH)
        pl.semaphore_wait(barrier, group)
        mine = me % group

        def copy(k):
            i = (mine + k) % group
            return pltpu.make_async_remote_copy(
                src_ref=rest.at[i], dst_ref=landing.at[mine], send_sem=send_sem.at[k],
                recv_sem=recv_sem.at[k], device_id={"rows": base + i},
                device_id_type=pl.DeviceIdType.MESH)

        for k in range(group):
            copy(k).start()
        for k in range(group):
            copy(k).wait()


def swapped(n, rest, after):
    dma = pltpu.SemaphoreType.DMA
    group = rest.shape[0]
    return pl.pallas_call(
        functools.partial(swap, n),
        out_shape=pltpu.VMEM(rest.shape, BF16),
        in_specs=[pl.BlockSpec(memory_space=pltpu.VMEM)] * 2,
        out_specs=pl.BlockSpec(memory_space=pltpu.VMEM),
        scratch_shapes=[dma((group,)), dma((group,))],
        compiler_params=pltpu.CompilerParams(
            collective_id=1, has_side_effects=True, vmem_limit_bytes=1024 * 1024),
    )(rest, after)


def add(n, ready, landing, result, sem):
    _, group, quarter, inner = place(n)

    @pl.when(inner)
    def _():
        at = pl.ds(pl.multiple_of((3 - quarter) * group, group), group)
        copy = pltpu.make_async_copy(landing, result.at[result.shape[0] - 1, at], sem)
        copy.start()
        copy.wait()


def added(n, ready, landing):
    hbm = pl.BlockSpec(memory_space=pl.ANY)
    return pl.pallas_call(
        functools.partial(add, n),
        out_shape=jax.ShapeDtypeStruct(ready.shape, ready.dtype),
        in_specs=[hbm, pl.BlockSpec(memory_space=pltpu.VMEM)],
        out_specs=hbm,
        scratch_shapes=[pltpu.SemaphoreType.DMA(())],
        input_output_aliases={0: 0},
        compiler_params=pltpu.CompilerParams(vmem_limit_bytes=1024 * 1024),
    )(ready, landing)


def per_device(n, owners, train_gate, other_gate, train_up, other_up, router_weight, router_gain):
    experts, rows, width = train_gate.shape
    each = experts // n
    units = 2 * each
    half = n // 2
    part = rows // PARTS
    deep = FAR_DEEP + NEAR_DEEP
    columns = router_weight.shape[1]
    blocks = [x.reshape(n, each, rows, width) for x in (train_gate, other_gate, train_up, other_up)]
    hbm, vmem = pl.BlockSpec(memory_space=pl.ANY), pl.BlockSpec(memory_space=pltpu.VMEM)
    dma = pltpu.SemaphoreType.DMA
    scratch = n * rows * width * 12 + deep * part * width * 2 + units * (3 * half + 2) * 2 * width * 4
    results = pl.pallas_call(
        functools.partial(kernel, n, owners, each),
        out_shape=(
            pltpu.VMEM((each, n, rows, width), BF16),
            pltpu.VMEM((each, n, rows, width), BF16),
            pltpu.VMEM((each, width), F32),
            pltpu.VMEM((each, width), F32),
            pltpu.VMEM((n * rows, owners * columns), BF16),
            pltpu.VMEM((n // 4, rows, width), BF16),
        ),
        in_specs=[hbm] * 4 + [pl.BlockSpec(memory_space=pltpu.HBM)] * 2,
        out_specs=(vmem,) * 6,
        scratch_shapes=[
            pltpu.VMEM((2, n, rows, width), F32),
            pltpu.VMEM((2, n, rows, width), BF16),
            pltpu.VMEM((deep, part, width), BF16),
            pltpu.VMEM((units, half, 2, width), F32),
            pltpu.VMEM((units, half, 2, width), F32),
            pltpu.VMEM((units, 2, width), F32),
            pltpu.VMEM((units, 2, width), F32),
            pltpu.VMEM((units, half, 2, width), F32),
            pltpu.VMEM((n, 1, width), F32),
            pltpu.VMEM((n, 1, width), F32),
            pltpu.VMEM((columns, rows), F32),
            pltpu.VMEM((1, rows), F32),
            pltpu.VMEM((rows, owners * columns), BF16),
            pltpu.VMEM((owners, rows, owners * columns), BF16),
            dma((2, half, 2)), dma((deep,)), dma((2, n)), pltpu.SemaphoreType.REGULAR,
            dma((n,)), dma((n,)), dma((2,)),
            dma((half,)), dma((half,)), dma((2,)), dma((2,)), dma((half,)), dma((half,)),
            dma((owners,)), dma((owners,)), dma((half,)), dma((half,)), dma(()), dma(()),
            dma((owners,)), dma((owners,)), dma((half,)), dma((half,)),
        ],
        compiler_params=pltpu.CompilerParams(
            collective_id=0, has_side_effects=True, vmem_limit_bytes=scratch + 4 * 1024 * 1024
        ),
    )(*blocks, router_weight.T, router_gain.reshape(1, rows))
    ready_gate, ready_up, scale_gate, scale_up, router, token = stored(n, results[:5])
    landing = swapped(n, results[5], token)
    ready_up = added(n, ready_up, landing)
    ready_gate, ready_up = (x.reshape(each, n * rows, width) for x in (ready_gate, ready_up))
    return (ready_gate, ready_up, scale_gate, scale_up, router)


def solution(mesh):
    n, owners = mesh.shape["rows"], mesh.shape["owner"]
    in_specs = (
        P("owner", "rows", None),
        P("owner", "rows", None),
        P("owner", "rows", None),
        P("owner", "rows", None),
        P("rows", "owner"),
        P("rows"),
    )
    out_specs = (
        P(("owner", "rows"), None, None),
        P(("owner", "rows"), None, None),
        P(("owner", "rows"), None),
        P(("owner", "rows"), None),
        P(),
    )
    return jax.shard_map(
        functools.partial(per_device, n, owners), mesh=mesh, in_specs=in_specs,
        out_specs=out_specs, check_vma=False,
    )
```

```python
import functools

import jax
import jax.numpy as jnp
from jax import lax
from jax.experimental import pallas as pl
from jax.experimental.pallas import tpu as pltpu
from jax.sharding import PartitionSpec as P

F32, BF16 = jnp.float32, jnp.bfloat16
VMEM_BYTES = 67_043_328
CHUNK = 32
PARTS, FAR_DEEP, NEAR_DEEP, SPLIT, COMMON = 4, 3, 4, 2, 6


def flipped(me, k, n):
    out, bit = 0, 1
    while bit < n:
        out = out + ((me // bit + k // bit) % 2) * bit
        bit *= 2
    return out


def kernel(n, owners, each, train_gate, other_gate, train_up, other_up, router_weight, router_gain,
           ready_gate, ready_up, scale_gate, scale_up, router, rest,
           wide, narrow, send, maxes, gathered, halves, mirrored, full, solo, direct,
           weight, gain, padded, pieces,
           load_sem, send_sem, recv_sem, gate_sem, ds_sem, dr_sem, router_sem,
           as_sem, ar_sem, bs_sem, br_sem, cs_sem, cr_sem,
           r1_send, r1_recv, r2_send, r2_recv, r3_send, r3_recv, r4_send, r4_recv, r5_send, r5_recv):
    me, owner = lax.axis_index("rows"), lax.axis_index("owner")
    rows = wide.shape[2]
    units = 2 * each
    half = n // 2
    spot = me % half
    base = me - spot
    mirror = (me + half) % n
    deep = send.shape[0]
    part = send.shape[1]
    parts = rows // part
    trains, others, readies = (train_gate, train_up), (other_gate, other_up), (ready_gate, ready_up)
    scales = (scale_gate, scale_up)

    def remote(src, dst, s, r, **where):
        return pltpu.make_async_remote_copy(
            src_ref=src, dst_ref=dst, send_sem=s, recv_sem=r, device_id=where,
            device_id_type=pl.DeviceIdType.MESH,
        )

    def loads(unit, q):
        kind, j, slot = unit // each, unit % each, unit % 2
        two = pl.ds(2 * q, 2)
        return (
            pltpu.make_async_copy(trains[kind].at[two, j], wide.at[slot, two], load_sem.at[slot, q, 0]),
            pltpu.make_async_copy(others[kind].at[two, j], narrow.at[slot, two], load_sem.at[slot, q, 1]),
        )

    def pair(k):
        return (spot + k) % half

    def start(unit):
        if unit < units:
            def one(k, _):
                for copy in loads(unit, pair(k)):
                    copy.start()
                return 0

            lax.fori_loop(1, half + 1, one, 0)

    start(0)
    barrier = pltpu.get_barrier_semaphore()
    for k in range(1, n):
        pl.semaphore_signal(barrier, inc=1, device_id={"rows": (me + k) % n},
                            device_id_type=pl.DeviceIdType.MESH)
    for k in range(1, owners):
        pl.semaphore_signal(barrier, inc=1, device_id={"owner": (owner + k) % owners},
                            device_id_type=pl.DeviceIdType.MESH)
    routing = (pltpu.make_async_copy(router_weight, weight, router_sem.at[0]),
               pltpu.make_async_copy(router_gain, gain, router_sem.at[1]))
    for copy in routing:
        copy.start()

    def to_spot(unit, k):
        q = pair(k)
        return remote(maxes.at[unit, q], gathered.at[unit, spot], as_sem.at[k],
                      ar_sem.at[k], rows=base + q)

    def to_mirror(unit):
        return remote(halves.at[unit], mirrored.at[unit], bs_sem.at[unit % 2], br_sem.at[unit % 2], rows=mirror)

    def to_half(unit, k):
        return remote(full.at[unit, spot], full.at[unit, spot], cs_sem.at[k],
                      cr_sem.at[k], rows=base + pair(k))

    def maxima(unit):
        slot = unit % 2

        def largest(d):
            acc = None
            for i in range(rows // CHUNK):
                x = wide[slot, d, i * CHUNK:(i + 1) * CHUNK, :]
                y = narrow[slot, d, i * CHUNK:(i + 1) * CHUNK, :].astype(F32)
                a = jnp.abs(x + y)
                acc = a if acc is None else jnp.maximum(acc, a)
            return jnp.max(acc, axis=0, keepdims=True)

        def both(k, _):
            q = pair(k)
            for copy in loads(unit, q):
                copy.wait()
            for s in range(2):
                d = 2 * q + s
                most = largest(d)
                maxes[unit, q, s:s + 1, :] = most
                if unit == 0:
                    solo[d] = most
            return 0

        def shared(k, _):
            both(k, 0)
            if unit > 0:
                to_spot(unit, k).start()
            return 0

        lax.fori_loop(1, half, shared, 0)
        both(0, 0)
        gathered[unit, spot] = maxes[unit, spot]
        if unit == 0:
            direct[me] = solo[mirror]

    def to_direct(k):
        r = (me + k) % n
        return remote(solo.at[(r + half) % n], direct.at[me], ds_sem.at[k], dr_sem.at[k], rows=r)

    def first_scale():
        for k in range(1, n):
            to_direct(k).wait()
        total = direct[0]
        for d in range(1, n):
            total = jnp.maximum(total, direct[d])
        return total

    def across(unit):
        for k in range(1, half):
            to_spot(unit, k).wait()
        mine = gathered[unit, 0]
        for q in range(1, half):
            mine = jnp.maximum(mine, gathered[unit, q])
        halves[unit] = mine
        to_mirror(unit).start()

    def spread(unit):
        to_mirror(unit).wait()
        full[unit, spot] = jnp.maximum(halves[unit], mirrored[unit])
        for k in range(1, half):
            to_half(unit, k).start()

    def known(unit):
        kind, j = unit // each, unit % each
        for k in range(1, half):
            to_half(unit, k).wait()
        scales[kind][j:j + 1, :] = scale_of(unit, me)

    def scale_of(unit, d):
        two = full[unit, d // 2]
        return jnp.where(d % 2 == 0, two[0:1], two[1:2])

    far_items, near_items = half * parts, (half - 2) * parts
    late = far_items // 2
    side = me % 2
    quarter = me // (half // 2)
    inner = jnp.logical_or(quarter == 1, quarter == 2)

    def far_count(unit):
        return far_items if unit < units - 2 else far_items - late

    def far_base(unit):
        return sum(far_count(u) for u in range(unit))

    def item_count(unit):
        return far_count(unit) + near_items + parts

    def item(unit, t):
        lead = parts if unit == 0 else 0
        mixed = far_count(unit) - lead + near_items
        after = jnp.maximum(t - lead, 0)
        phase = side * (2 * mixed // 3)
        near_at = (after * near_items + phase) // mixed
        leading, beside = t < lead, t >= lead + mixed
        is_far = jnp.logical_or(leading, jnp.logical_and(
            jnp.logical_not(beside), ((after + 1) * near_items + phase) // mixed == near_at))
        far_at = jnp.where(leading, t, lead + after - near_at)
        near_at = jnp.where(beside, near_items + t - lead - mixed, near_at)
        at = jnp.where(is_far, far_at, near_at)
        near_k = jnp.where(beside, 1, 2 + at // parts)
        d = flipped(me, jnp.where(is_far, half + at // parts, near_k), n)
        slot = jnp.where(is_far, (far_base(unit) + far_at) % FAR_DEEP,
                         FAR_DEEP + (unit * (near_items + parts) + near_at) % NEAR_DEEP)
        fresh = at < jnp.where(is_far, FAR_DEEP, NEAR_DEEP)
        return d, at % parts, slot, fresh

    def part_of(piece):
        return pl.ds(pl.multiple_of(piece * part, part), part)

    def data(unit, d, piece, slot):
        kind, j = unit // each, unit % each
        return remote(send.at[slot], readies[kind].at[j, me, part_of(piece)], send_sem.at[slot],
                      recv_sem.at[kind, me], rows=d)

    def scaled(unit, d, piece, put, scale=None):
        inverse = 1.0 / (scale_of(unit, d) if scale is None else scale)
        chunk = min(CHUNK, part)
        for i in range(part // chunk):
            at = pl.ds(pl.multiple_of(piece * part + i * chunk, chunk), chunk)
            x = wide[unit % 2, d, at, :]
            y = narrow[unit % 2, d, at, :].astype(F32)
            put(i * chunk, chunk, ((x + y) * inverse).astype(BF16))

    def issue(unit, first, last, scale=None):
        def one(t, _):
            d, piece, slot, fresh = item(unit, t)
            if unit == 0:
                @pl.when(jnp.logical_not(fresh))
                def _():
                    data(unit, d, piece, slot).wait_send()
            else:
                data(unit, d, piece, slot).wait_send()

            def put(at, size, value):
                send[slot, at:at + size, :] = value

            scaled(unit, d, piece, put, scale)
            data(unit, d, piece, slot).start()
            return 0

        lax.fori_loop(first, last, one, 0)

    def late_item(unit, t):
        far_at = far_items - late + t
        d = flipped(me, half + far_at // parts, n)
        return d, far_at % parts, (far_base(units) + t) % FAR_DEEP

    def issue_late(unit, first, last):
        def one(t, _):
            d, piece, slot = late_item(unit, t)
            slot = slot if unit == units - 2 else (slot + late) % FAR_DEEP
            data(unit, d, piece, slot).wait_send()

            def put(at, size, value):
                send[slot, at:at + size, :] = value

            scaled(unit, d, piece, put)
            data(unit, d, piece, slot).start()
            return 0

        lax.fori_loop(first, last, one, 0)

    def leave(unit):
        def one(t, _):
            d, piece, _ = late_item(unit, t)

            def put(at, size, value):
                rest[d % (half // 2), pl.ds(pl.multiple_of(piece * part + at, size), size), :] = value

            scaled(unit, d, piece, put)
            return 0

        lax.fori_loop(0, late, one, 0)

    def own(unit):
        kind, j = unit // each, unit % each

        def one(piece, _):
            def put(at, size, value):
                readies[kind][j, me, pl.ds(pl.multiple_of(piece * part + at, size), size), :] = value

            scaled(unit, me, piece, put)
            return 0

        lax.fori_loop(0, parts, one, 0)

    rows_of = rows // owners

    def block_of(r):
        return pl.ds(pl.multiple_of(r * rows, rows), rows)

    def share_of(r, o):
        return pl.ds(pl.multiple_of(r * rows + o * rows_of, rows_of), rows_of)

    def r1(k):
        return remote(padded, pieces.at[owner], r1_send.at[k], r1_recv.at[k], owner=(owner + k) % owners)

    def r2(k):
        at = router.at[block_of(me)]
        return remote(at, at, r2_send.at[k], r2_recv.at[k], rows=base + pair(k))

    def r3():
        at = router.at[share_of(me, owner)]
        return remote(at, at, r3_send, r3_recv, rows=mirror)

    def r4(k):
        at = router.at[share_of(mirror, owner)]
        return remote(at, at, r4_send.at[k], r4_recv.at[k], owner=(owner + k) % owners)

    def r5(k):
        at = router.at[block_of(mirror)]
        return remote(at, at, r5_send.at[k], r5_recv.at[k], rows=base + pair(k))

    def router_owners():
        for copy in routing:
            copy.wait()
        columns, lanes = weight.shape[0], padded.shape[1]
        lane = lax.broadcasted_iota(jnp.int32, (columns, lanes), 1)
        row = lax.broadcasted_iota(jnp.int32, (columns, lanes), 0)
        place = (lane == row + owner * columns).astype(F32).astype(BF16)
        mine = (weight[...] * gain[...]).astype(BF16)
        padded[...] = lax.dot_general(mine, place, (((0,), (0,)), ((), ())),
                                      preferred_element_type=F32).astype(BF16)
        pieces[owner] = padded[...]
        for k in range(1, owners):
            r1(k).start()

    def router_rows():
        for k in range(1, owners):
            r1(k).wait()
        total = pieces[0].astype(F32)
        for o in range(1, owners):
            total = total + pieces[o].astype(F32)
        router[block_of(me), :] = total.astype(BF16)
        r3().start()
        for k in range(1, half):
            r2(k).start()

    def router_across():
        r3().wait()
        for k in range(1, owners):
            r4(k).start()

    def router_far():
        for k in range(1, owners):
            r4(k).wait()
        for k in range(1, half):
            r5(k).start()

    maxima(0)
    pl.semaphore_wait(barrier, n - 1 + owners - 1)
    for k in range(1, half):
        to_spot(0, k).start()
    for k in range(1, n):
        to_direct(k).start()
    start(1)
    across(0)
    now = min(FAR_DEEP, parts)
    first = first_scale()
    issue(0, 0, now, first)
    spread(0)
    issue(0, now, parts, first)
    known(0)
    stages = [router_owners, router_rows, router_across, router_far]
    steps = (maxima, across, spread)
    for unit in range(units):
        more = unit + 1 < units
        at = parts if unit == 0 else 0
        items = item_count(unit)
        marks = [at + (items - at) * mark // 28 for mark in (2, 9, 16)]
        for mark, step in zip(marks, steps):
            issue(unit, at, mark)
            at = mark
            if more:
                step(unit + 1)
        issue(unit, at, items)
        own(unit)
        start(unit + 2)
        if more:
            known(unit + 1)
        if stages:
            stages.pop(0)()
    for stage in stages:
        stage()
    def sent(slot):
        data(0, mirror, 0, slot).wait_send()

    common = late * COMMON // 8
    issue_late(units - 2, 0, common)

    @pl.when(inner)
    def _():
        issue_late(units - 2, common, late)
        for t in range(late - FAR_DEEP, late - 1):
            sent((far_base(units) + t) % FAR_DEEP)
        for k in range(half // 2, half):
            pl.semaphore_signal(gate_sem, inc=1, device_id={"rows": flipped(me, k, n)},
                                device_id_type=pl.DeviceIdType.MESH)
        leave(units - 1)
        sent((far_base(units) + late - 1) % FAR_DEEP)

    @pl.when(jnp.logical_not(inner))
    def _():
        pl.semaphore_wait(gate_sem, half // 2)
        issue_late(units - 2, common, late)
        issue_late(units - 1, 0, late)
        for slot in range(FAR_DEEP):
            sent(slot)

    for k in range(1, half):
        r2(k).wait()
        r5(k).wait()
    for slot in range(FAR_DEEP, deep):
        sent(slot)

    def landed(kind, d, count):
        at = readies[kind].at[pl.ds(0, count), d]
        remote(at, at, send_sem.at[0], recv_sem.at[kind, d], rows=d).wait_recv()

    def all_of(kind):
        def one(k, _):
            landed(kind, flipped(me, k, n), each)
            return 0
        return one

    lax.fori_loop(1, n, all_of(0), 0)
    lax.fori_loop(1, n - half // 2, all_of(1), 0)

    @pl.when(jnp.logical_not(inner))
    def _():
        lax.fori_loop(n - half // 2, n, all_of(1), 0)

    if each > 1:
        @pl.when(inner)
        def _():
            def one(k, _):
                landed(1, flipped(me, k, n), each - 1)
                return 0

            lax.fori_loop(n - half // 2, n, one, 0)


def place(n):
    me = lax.axis_index("rows")
    group = n // 4
    quarter = me // group
    return me, group, quarter, jnp.logical_or(quarter == 1, quarter == 2)


def store(n, *refs):
    count = (len(refs) - 2) // 2
    sources, results, token, sem = refs[:count], refs[count:2 * count], refs[2 * count], refs[2 * count + 1]
    token[...] = jnp.zeros_like(token)
    _, group, quarter, inner = place(n)
    copies = []

    def copy(i, index=None):
        pieces = (sources[i], results[i]) if index is None else (sources[i].at[index], results[i].at[index])
        made = pltpu.make_async_copy(*pieces, sem.at[len(copies)])
        copies.append(made)
        return made

    each = sources[0].shape[0]
    size = n // SPLIT
    whole = [copy(i) for i in range(2, count)]
    for i in range(2):
        for j in range(each if i == 0 else each - 1):
            whole += [copy(i, (j, pl.ds(at * size, size))) for at in range(SPLIT)]
    last = [copy(1, (each - 1, pl.ds(c * group, group))) for c in range(4)]
    for made in whole:
        made.start()

    def guarded(act):
        for c, made in enumerate(last):
            @pl.when(jnp.logical_not(jnp.logical_and(inner, quarter == 3 - c)))
            def _(made=made):
                act(made)

    guarded(lambda made: made.start())
    for made in whole:
        made.wait()
    guarded(lambda made: made.wait())


def stored(n, arrays):
    count = len(arrays)
    copies = count - 2 + (2 * arrays[0].shape[0] - 1) * SPLIT + 4
    return pl.pallas_call(
        functools.partial(store, n),
        out_shape=tuple(jax.ShapeDtypeStruct(x.shape, x.dtype) for x in arrays) + (pltpu.VMEM((8, 128), F32),),
        in_specs=[pl.BlockSpec(memory_space=pltpu.VMEM)] * count,
        out_specs=(pl.BlockSpec(memory_space=pl.ANY),) * count + (pl.BlockSpec(memory_space=pltpu.VMEM),),
        scratch_shapes=[pltpu.SemaphoreType.DMA((copies,))],
        compiler_params=pltpu.CompilerParams(vmem_limit_bytes=1024 * 1024),
    )(*arrays)


def swap(n, rest, _, landing, send_sem, recv_sem):
    me, group, quarter, inner = place(n)
    base = (3 - quarter) * group

    @pl.when(inner)
    def _():
        barrier = pltpu.get_barrier_semaphore()
        for i in range(group):
            pl.semaphore_signal(barrier, inc=1, device_id={"rows": base + i},
                                device_id_type=pl.DeviceIdType.MESH)
        pl.semaphore_wait(barrier, group)
        mine = me % group

        def copy(k):
            i = (mine + k) % group
            return pltpu.make_async_remote_copy(
                src_ref=rest.at[i], dst_ref=landing.at[mine], send_sem=send_sem.at[k],
                recv_sem=recv_sem.at[k], device_id={"rows": base + i},
                device_id_type=pl.DeviceIdType.MESH)

        for k in range(group):
            copy(k).start()
        for k in range(group):
            copy(k).wait()


def swapped(n, rest, after):
    dma = pltpu.SemaphoreType.DMA
    group = rest.shape[0]
    return pl.pallas_call(
        functools.partial(swap, n),
        out_shape=pltpu.VMEM(rest.shape, BF16),
        in_specs=[pl.BlockSpec(memory_space=pltpu.VMEM)] * 2,
        out_specs=pl.BlockSpec(memory_space=pltpu.VMEM),
        scratch_shapes=[dma((group,)), dma((group,))],
        compiler_params=pltpu.CompilerParams(
            collective_id=1, has_side_effects=True, vmem_limit_bytes=1024 * 1024),
    )(rest, after)


def add(n, ready, landing, result, sem):
    _, group, quarter, inner = place(n)

    @pl.when(inner)
    def _():
        at = pl.ds(pl.multiple_of((3 - quarter) * group, group), group)
        copy = pltpu.make_async_copy(landing, result.at[result.shape[0] - 1, at], sem)
        copy.start()
        copy.wait()


def added(n, ready, landing):
    hbm = pl.BlockSpec(memory_space=pl.ANY)
    return pl.pallas_call(
        functools.partial(add, n),
        out_shape=jax.ShapeDtypeStruct(ready.shape, ready.dtype),
        in_specs=[hbm, pl.BlockSpec(memory_space=pltpu.VMEM)],
        out_specs=hbm,
        scratch_shapes=[pltpu.SemaphoreType.DMA(())],
        input_output_aliases={0: 0},
        compiler_params=pltpu.CompilerParams(vmem_limit_bytes=1024 * 1024),
    )(ready, landing)


def per_device(n, owners, train_gate, other_gate, train_up, other_up, router_weight, router_gain):
    experts, rows, width = train_gate.shape
    each = experts // n
    units = 2 * each
    half = n // 2
    part = rows // PARTS
    deep = FAR_DEEP + NEAR_DEEP
    columns = router_weight.shape[1]
    blocks = [x.reshape(n, each, rows, width) for x in (train_gate, other_gate, train_up, other_up)]
    hbm, vmem = pl.BlockSpec(memory_space=pl.ANY), pl.BlockSpec(memory_space=pltpu.VMEM)
    dma = pltpu.SemaphoreType.DMA
    held = 2 * n * rows * (2 * each * width + owners * columns) + 8 * each * width + n // 4 * rows * width * 2
    results = pl.pallas_call(
        functools.partial(kernel, n, owners, each),
        out_shape=(
            pltpu.VMEM((each, n, rows, width), BF16),
            pltpu.VMEM((each, n, rows, width), BF16),
            pltpu.VMEM((each, width), F32),
            pltpu.VMEM((each, width), F32),
            pltpu.VMEM((n * rows, owners * columns), BF16),
            pltpu.VMEM((n // 4, rows, width), BF16),
        ),
        in_specs=[hbm] * 4 + [pl.BlockSpec(memory_space=pltpu.HBM)] * 2,
        out_specs=(vmem,) * 6,
        scratch_shapes=[
            pltpu.VMEM((2, n, rows, width), F32),
            pltpu.VMEM((2, n, rows, width), BF16),
            pltpu.VMEM((deep, part, width), BF16),
            pltpu.VMEM((units, half, 2, width), F32),
            pltpu.VMEM((units, half, 2, width), F32),
            pltpu.VMEM((units, 2, width), F32),
            pltpu.VMEM((units, 2, width), F32),
            pltpu.VMEM((units, half, 2, width), F32),
            pltpu.VMEM((n, 1, width), F32),
            pltpu.VMEM((n, 1, width), F32),
            pltpu.VMEM((columns, rows), F32),
            pltpu.VMEM((1, rows), F32),
            pltpu.VMEM((rows, owners * columns), BF16),
            pltpu.VMEM((owners, rows, owners * columns), BF16),
            dma((2, half, 2)), dma((deep,)), dma((2, n)), pltpu.SemaphoreType.REGULAR,
            dma((n,)), dma((n,)), dma((2,)),
            dma((half,)), dma((half,)), dma((2,)), dma((2,)), dma((half,)), dma((half,)),
            dma((owners,)), dma((owners,)), dma((half,)), dma((half,)), dma(()), dma(()),
            dma((owners,)), dma((owners,)), dma((half,)), dma((half,)),
        ],
        compiler_params=pltpu.CompilerParams(
            collective_id=0, has_side_effects=True, vmem_limit_bytes=VMEM_BYTES - held - 8192
        ),
    )(*blocks, router_weight.T, router_gain.reshape(1, rows))
    ready_gate, ready_up, scale_gate, scale_up, router, token = stored(n, results[:5])
    landing = swapped(n, results[5], token)
    ready_up = added(n, ready_up, landing)
    ready_gate, ready_up = (x.reshape(each, n * rows, width) for x in (ready_gate, ready_up))
    return (ready_gate, ready_up, scale_gate, scale_up, router)


def solution(mesh):
    n, owners = mesh.shape["rows"], mesh.shape["owner"]
    in_specs = (
        P("owner", "rows", None),
        P("owner", "rows", None),
        P("owner", "rows", None),
        P("owner", "rows", None),
        P("rows", "owner"),
        P("rows"),
    )
    out_specs = (
        P(("owner", "rows"), None, None),
        P(("owner", "rows"), None, None),
        P(("owner", "rows"), None),
        P(("owner", "rows"), None),
        P(),
    )
    return jax.shard_map(
        functools.partial(per_device, n, owners), mesh=mesh, in_specs=in_specs,
        out_specs=out_specs, check_vma=False,
    )
```
